32 devices in a mesh: batch: 2 (over x), row: 4 (over z), col: 4 (over y, core).
Axes of the slice: x: 2, y: 2, z: 4, core: 2. Of those that a mesh axis runs over, the one named last changes fastest.
Arguments:
- operator: bfloat16 [12288, 6144], P(('batch', 'row'), 'col'), parts along dimension 0
- start_block: float32 [12288, 256], P(('batch', 'row', 'col')), parts along dimension 0
- shifts: float32 [32], P('batch'), parts along dimension 0
Outputs:
- output 1: float32 [12288, 256], P(('batch', 'row', 'col')), parts along dimension 0
- output 2: float32 [512, 256], P('batch'), parts along dimension 0
There are 2 independent parts. The reference program is written for one: setup_inputs(seed, part) draws one part's arguments, and reference() takes and returns one part's arrays. A program takes and returns all parts, laid end to end along the dimension named above; each array names one.
All inputs are finite; a program needn't handle non-finite values.
Results may differ from the reference program's by a relative error of at most 0.001.
Values are sent between devices in bfloat16 or wider.
A program may use at most 1 GiB of HBM per device.

```python
import jax
import jax.numpy as jnp
from jax import lax

MAT_ORDER = 6144
BLOCK_COLS = 256
SWEEPS = 16


def setup_inputs(seed: int = 0, part: int = 0) -> dict:
    key = jax.random.fold_in(jax.random.key(seed), part)
    key_basis, key_noise, key_start, key_shift = jax.random.split(key, 4)
    basis = jnp.linalg.qr(jax.random.normal(key_basis, (MAT_ORDER, BLOCK_COLS), jnp.float32))[0]
    levels = 10.0 ** (jnp.arange(BLOCK_COLS, dtype=jnp.float32) / (BLOCK_COLS - 1))
    noise = jax.random.normal(key_noise, (MAT_ORDER, MAT_ORDER), jnp.float32)
    spread = 0.2 * (2.0 * MAT_ORDER) ** -0.5
    operator = jnp.dot(basis * levels, basis.T) + spread * (noise + noise.T)
    start_block = jax.random.normal(key_start, (MAT_ORDER, BLOCK_COLS), jnp.float32)
    shifts = jax.random.uniform(key_shift, (SWEEPS,), jnp.float32, -0.5, 0.1)
    return {"operator": operator.astype(jnp.bfloat16), "start_block": start_block, "shifts": shifts}


def cholesky_solve(block, gram):
    lower = jnp.linalg.cholesky(gram)
    return lax.linalg.triangular_solve(lower, block, left_side=False, lower=True, transpose_a=True)


def orthonormalize(block):
    block_low = block.astype(jnp.bfloat16)
    gram_one = jnp.dot(block_low.T, block_low, preferred_element_type=jnp.float32)
    block = cholesky_solve(block, gram_one)
    gram_two = jnp.dot(block.T, block, precision=lax.Precision.HIGHEST, preferred_element_type=jnp.float32)
    return cholesky_solve(block, gram_two)


def reference(operator, start_block, shifts):
    def sweep(block, shift):
        image = jnp.dot(operator, block.astype(jnp.bfloat16), preferred_element_type=jnp.float32)
        return orthonormalize(image - shift * block), None
    block = lax.scan(sweep, start_block, shifts)[0]
    final_image = jnp.dot(operator, block.astype(jnp.bfloat16), preferred_element_type=jnp.float32)
    rayleigh = jnp.dot(block.T, final_image, precision=lax.Precision.HIGHEST, preferred_element_type=jnp.float32)
    return block, rayleigh
```

```python
import functools
import jax, jax.numpy as jnp
from jax import lax
from jax.experimental import pallas as pl
from jax.experimental.pallas import tpu as pltpu
HIGHEST = lax.Precision.HIGHEST
N = 256; NB = 16; LANES = 128

def dot(a, b, dims=((1,), (0,))):
    return lax.dot_general(a, b, (dims, ((), ())), precision=HIGHEST, preferred_element_type=jnp.float32)

def inverse_factor(w, out, qpad):
    rows = lax.broadcasted_iota(jnp.int32, (NB, LANES), 0)
    lanes = lax.broadcasted_iota(jnp.int32, (NB, LANES), 1)
    qpad[...] = jnp.zeros_like(qpad)
    for k in range(0, N, NB):
        grp, off = k // LANES, k % LANES
        panel = [w[k:k+NB, g*LANES:(g+1)*LANES] for g in range(2)]
        cols = [jnp.broadcast_to(panel[grp][:, off+m:off+m+1], (NB, LANES)) for m in range(NB)]
        for j in range(NB):
            here = rows == j
            pivot = cols[j][j:j+1, :]
            inv = 1.0 / pivot
            root = lax.rsqrt(pivot)
            panel[grp] = jnp.where(lanes == off + j, here.astype(jnp.float32), panel[grp])
            coef = cols[j]
            for g in range(2):
                row = panel[g][j:j+1, :]
                out[k+j:k+j+1, g*LANES:(g+1)*LANES] = jnp.where(
                    lax.broadcasted_iota(jnp.int32, (1, LANES), 1) + g*LANES <= k + j, row * root, 0.0)
                q = row * inv
                panel[g] = jnp.where(here, q, panel[g] - coef * q)
            for m in range(j+1, NB):
                q = cols[m][j:j+1, :] * inv
                cols[m] = jnp.where(here, q, cols[m] - coef * q)
        if k + NB < N:
            if off >= NB:
                qpad[off-NB:off, :] = jnp.zeros((NB, N), jnp.float32)
            elif k:
                qpad[LANES-NB:LANES, :] = jnp.zeros((NB, N), jnp.float32)
            for g in range(2):
                qpad[off:off+NB, g*LANES:(g+1)*LANES] = panel[g]
            q = qpad[...]
            pieces = [(k+NB, k+2*NB)]
            if k + 2*NB < N:
                pieces.append((k+2*NB, N))
            for lo, hi in pieces:
                lhs = w[lo:hi, grp*LANES:(grp+1)*LANES]
                t = dot(lhs, q)
                lane = lax.broadcasted_iota(jnp.int32, (hi-lo, N), 1)
                old = w[lo:hi, :]
                w[lo:hi, :] = jnp.where((lane >= k) & (lane < k+NB), 0.0, old) - t

def kernel(g1, s, y, x, w, inv1, inv2, qpad):
    w[...] = g1[...]
    inverse_factor(w, inv1, qpad)
    a = inv1[...]
    w[...] = dot(dot(a, s[...]), a, ((1,), (1,)))
    inverse_factor(w, inv2, qpad)
    n = dot(inv2[...], a)
    x[...] = dot(y[...], n, ((1,), (1,)))

def solve(g1, s, y):
    v = pltpu.VMEM
    return pl.pallas_call(kernel, out_shape=jax.ShapeDtypeStruct(y.shape, jnp.float32),
        in_specs=[pl.BlockSpec(memory_space=pltpu.VMEM)]*3, out_specs=pl.BlockSpec(memory_space=pltpu.VMEM),
        scratch_shapes=[v((N,N),jnp.float32)]*3+[v((LANES,N),jnp.float32)], name="solve")(g1, s, y)


def solution(mesh):
    from jax.sharding import PartitionSpec as P
    grid = ("row", "col")
    row_count, col_count = mesh.shape["row"], mesh.shape["col"]
    moves = [(i, (i % row_count) * col_count + i // row_count) for i in range(row_count * col_count)]

    def apply_block(op_block, x_local):
        x_moved = lax.ppermute(x_local.astype(jnp.bfloat16), grid, moves)
        x_column = lax.all_gather(x_moved, "row", axis=0, tiled=True)
        part_sum = jnp.dot(op_block, x_column, preferred_element_type=jnp.float32)
        return lax.psum_scatter(part_sum, "col", scatter_dimension=0, tiled=True)

    def local_program(op_block, x_local, shift_vals):
        def sweep(step, x_local):
            y_local = apply_block(op_block, x_local) - shift_vals[step] * x_local
            y_low = y_local.astype(jnp.bfloat16)
            gram_one = jnp.einsum("ka,kb->ab", y_low, y_low, preferred_element_type=jnp.float32)
            gram_full = jnp.einsum("ka,kb->ab", y_local, y_local, precision=HIGHEST, preferred_element_type=jnp.float32)
            grams = lax.psum(jnp.stack([gram_one, gram_full]), grid)
            return solve(grams[0], grams[1], y_local)
        x_local = lax.fori_loop(0, shift_vals.shape[0], sweep, x_local)
        image = apply_block(op_block, x_local)
        local_gram = jnp.einsum("ka,kb->ab", x_local, image, precision=HIGHEST, preferred_element_type=jnp.float32)
        return x_local, lax.psum(local_gram, grid)

    return jax.shard_map(
        local_program, mesh=mesh,
        in_specs=(P(("batch", "row"), "col"), P(("batch", "row", "col"), None), P("batch")),
        out_specs=(P(("batch", "row", "col"), None), P("batch", None)),
        check_vma=False,
    )
```

```python
import functools

import jax
import jax.numpy as jnp
from jax import lax
from jax.experimental import pallas as pl
from jax.experimental.pallas import tpu as pltpu
from jax.sharding import PartitionSpec as P

HIGHEST = lax.Precision.HIGHEST
MESH = pl.DeviceIdType.MESH
LANES = 128
STEP = 16


def dot(a, b, dims=((1,), (0,))):
    return lax.dot_general(a, b, (dims, ((), ())), precision=HIGHEST, preferred_element_type=jnp.float32)


def inverse_factor(w, out, qpad, hook=None):
    n = w.shape[0]
    groups = n // LANES
    shape = (groups, STEP, LANES)
    rows = lax.broadcasted_iota(jnp.int32, (STEP, LANES), 0)
    spot = lax.broadcasted_iota(jnp.int32, shape, 0) * LANES + lax.broadcasted_iota(jnp.int32, shape, 2)
    qpad[...] = jnp.zeros_like(qpad)
    for k in range(0, n, STEP):
        if hook is not None:
            hook(k)
        grp, off = k // LANES, k % LANES
        panel = jnp.stack([w[k:k + STEP, g * LANES:(g + 1) * LANES] for g in range(groups)])
        cols = jnp.stack([jnp.broadcast_to(panel[grp][:, off + m:off + m + 1], (STEP, LANES)) for m in range(STEP)])
        done = []
        for j in range(STEP):
            here = (rows == j)[None]
            coef = cols[0]
            pivot = coef[j:j + 1, :]
            inv = 1.0 / pivot
            panel = jnp.where(spot == k + j, here.astype(jnp.float32), panel)
            row = panel[:, j:j + 1, :]
            done.append(row * lax.rsqrt(pivot))
            q = row * inv
            panel = jnp.where(here, q, panel - coef * q)
            if j + 1 < STEP:
                q = cols[1:, j:j + 1, :] * inv
                cols = jnp.where(here, q, cols[1:] - coef * q)
        done = jnp.concatenate(done, axis=1)
        low = k + lax.broadcasted_iota(jnp.int32, shape, 1)
        done = jnp.where(spot <= low, done, 0.0)
        for g in range(groups):
            out[k:k + STEP, g * LANES:(g + 1) * LANES] = done[g]
        if k + STEP == n:
            break
        if k:
            last = (k - STEP) % LANES
            qpad[last:last + STEP, :] = jnp.zeros((STEP, n), jnp.float32)
        for g in range(groups):
            qpad[off:off + STEP, g * LANES:(g + 1) * LANES] = panel[g]
        q = qpad[...]
        pieces = [(k + STEP, k + 2 * STEP)] + ([(k + 2 * STEP, n)] if k + 2 * STEP < n else [])
        for lo, hi in pieces:
            t = dot(w[lo:hi, grp * LANES:(grp + 1) * LANES], q)
            lane = lax.broadcasted_iota(jnp.int32, (hi - lo, n), 1)
            w[lo:hi, :] = jnp.where((lane >= k) & (lane < k + STEP), 0.0, w[lo:hi, :]) - t


class GroupSum:
    def __init__(self, part, bufs, sems, z, c):
        self.part, self.z, self.c = part, z, c
        self.one, self.two, self.out = bufs
        self.send, self.recv = sems

    def _copies(self, phase):
        me = self.z if phase == 1 else self.c
        for i in range(1, 4):
            peer = lax.rem(me + i, 4)
            src = (self.part.at[peer], self.two.at[me], self.out.at[me])[phase]
            dst = (self.one, self.two, self.out)[phase].at[me]
            yield pltpu.make_async_remote_copy(
                src_ref=src, dst_ref=dst, send_sem=self.send.at[phase, i], recv_sem=self.recv.at[phase, me],
                device_id={"row": peer} if phase == 1 else {"col": peer}, device_id_type=MESH)

    def _start(self, phase):
        for copy in self._copies(phase):
            copy.start()

    def _finish(self, phase):
        me = self.z if phase == 1 else self.c
        land = (self.one, self.two, self.out)[phase]
        for i in range(1, 4):
            src = lax.rem(me + i, 4)
            pltpu.make_async_copy(land.at[src], land.at[src], self.recv.at[phase, src]).wait()
        for copy in self._copies(phase):
            copy.wait_send()

    def begin(self):
        self._start(0)

    def middle(self):
        self._finish(0)
        self.one[self.c] = self.part[self.c]
        self.two[self.z] = (self.one[0] + self.one[1]) + (self.one[2] + self.one[3])
        self._start(1)

    def last(self):
        self._finish(1)
        self.out[self.c] = (self.two[0] + self.two[1]) + (self.two[2] + self.two[3])
        self._start(2)

    def end(self):
        self._finish(2)


def symmetric(ref):
    flat = ref[...].reshape(3 * LANES, LANES)
    a, b, c = flat[:LANES], flat[LANES:2 * LANES], flat[2 * LANES:]
    return a, b, b.T, c


def kernel(sweeps, a_hbm, x0, sigma, x_out, h_out, arows, xg, acc, xs, ys, w, inv1, inv2, qpad, full,
           part1, part2, part3, b11, b12, b13, b21, b22, b23, b31, b32, b33,
           asend, arecv, aown, up, down, zrecv, ysend, yrecv, dsend, drecv,
           s1, r1, s2, r2, s3, r3):
    z, c = lax.axis_index("row"), lax.axis_index("col")
    y, k = c // 2, lax.rem(c, 2)
    rb, bc = x0.shape
    half = rb // 2
    width = a_hbm.shape[1]
    twin = c + 1 - 2 * k
    across = lax.rem(c + 2, 4)

    barrier = pltpu.get_barrier_semaphore()
    for i in range(1, 4):
        pl.semaphore_signal(barrier, inc=1, device_id={"col": lax.rem(c + i, 4)}, device_id_type=MESH)
        pl.semaphore_signal(barrier, inc=1, device_id={"row": lax.rem(z + i, 4)}, device_id_type=MESH)
    pl.semaphore_wait(barrier, 6)

    def columns(block):
        return pl.ds(pl.multiple_of(block * width, LANES), width)

    def spread(i):
        peer = lax.rem(c + i, 4)
        return pltpu.make_async_remote_copy(
            src_ref=a_hbm.at[pl.ds(pl.multiple_of(peer * rb, STEP), rb)], dst_ref=arows.at[:, columns(c)],
            send_sem=asend.at[i], recv_sem=arecv.at[c], device_id={"col": peer}, device_id_type=MESH)

    own_rows = pltpu.make_async_copy(a_hbm.at[pl.ds(pl.multiple_of(c * rb, STEP), rb)], arows.at[:, columns(c)], aown)
    for i in range(1, 4):
        spread(i).start()
    own_rows.start()
    xs[...] = x0[...]
    own_rows.wait()
    for i in range(1, 4):
        src = lax.rem(c + i, 4)
        land = arows.at[:, columns(src)]
        pltpu.make_async_copy(land, land, arecv.at[src]).wait()
    for i in range(1, 4):
        spread(i).wait_send()

    def sweep(t, carry):
        p = lax.rem(t, 2)

        def shard(yy, zz, kk):
            return xg.at[p, zz * 4 + yy * 2 + kk]

        def piece(yy, zz, kk, h):
            return xg.at[p, zz * 4 + yy * 2 + kk, pl.ds(h * half, half)]

        def z_copy(zz, h, step):
            sems = up if step > 0 else down
            return pltpu.make_async_remote_copy(
                src_ref=piece(y, zz, k, h), dst_ref=piece(y, zz, k, h), send_sem=sems.at[zz, h],
                recv_sem=zrecv.at[zz, h], device_id={"row": z + step}, device_id_type=MESH)

        def y_copy(zz, h):
            return pltpu.make_async_remote_copy(
                src_ref=piece(y, zz, k, h), dst_ref=piece(y, zz, k, h), send_sem=ysend.at[zz, h],
                recv_sem=yrecv.at[zz, h], device_id={"col": across}, device_id_type=MESH)

        def d_copy(yy, zz):
            return pltpu.make_async_remote_copy(
                src_ref=shard(yy, zz, k), dst_ref=shard(yy, zz, k), send_sem=dsend.at[yy, zz],
                recv_sem=drecv.at[yy, zz], device_id={"col": twin}, device_id_type=MESH)

        def landed(ref, sem):
            pltpu.make_async_copy(ref, ref, sem).wait()

        def relay(act):
            for h in range(2):
                for step, ok in ((1, z < 3), (-1, z > 0)):
                    @pl.when(ok)
                    def _():
                        act(z_copy(z, h, step))
                act(y_copy(z, h))
            act(d_copy(y, z))
            for d in range(1, 4):
                for step, there, on in ((1, z >= d, z < 3), (-1, z + d <= 3, z > 0)):
                    @pl.when(there)
                    def _():
                        zz = z - step * d
                        for h in range(2):
                            if act is start:
                                landed(piece(y, zz, k, h), zrecv.at[zz, h])

                            @pl.when(on)
                            def _():
                                act(z_copy(zz, h, step))
                            act(y_copy(zz, h))
                        act(d_copy(y, zz))

        def start(copy):
            copy.start()

        def sent(copy):
            copy.wait_send()

        def near(i):
            return lax.rem(z // 2 + i // 2, 2) * 2 + lax.rem(lax.rem(z, 2) + lax.rem(i, 2), 2)

        def consume(yy, zz):
            block = zz * 4 + yy * 2
            cols = pl.ds(pl.multiple_of(block * rb, LANES), 2 * rb)
            acc[...] += jnp.dot(arows[:, cols], xg[p, pl.ds(block, 2)].reshape(2 * rb, bc), preferred_element_type=jnp.float32)

        xg[p, z * 4 + c] = xs[...].astype(jnp.bfloat16)
        relay(start)
        acc[...] = jnp.zeros_like(acc)

        def same_plane(i, carry):
            zz = near(i)
            landed(shard(y, zz, 1 - k), drecv.at[y, zz])
            consume(y, zz)
            return carry

        def other_plane(i, carry):
            zz = near(i)
            for h in range(2):
                landed(piece(1 - y, zz, k, h), yrecv.at[zz, h])
            d_copy(1 - y, zz).start()
            landed(shard(1 - y, zz, 1 - k), drecv.at[1 - y, zz])
            consume(1 - y, zz)
            return carry

        lax.fori_loop(0, 4, same_plane, 0)
        lax.fori_loop(0, 4, other_plane, 0)

        @pl.when(t < sweeps)
        def _():
            shift = sigma[lax.rem(t, sweeps)]
            yv = acc[...] - shift * xs[...]
            ys[...] = yv
            low = yv.astype(jnp.bfloat16)

            def lower(v, mul):
                v0, v1 = v[:, :LANES], v[:, LANES:]
                return [mul(a, b).reshape(LANES, LANES) for a, b in ((v0, v0), (v1, v0), (v1, v1))]

            def put(part, blocks):
                part[...] = jnp.concatenate(blocks, axis=0).reshape(part.shape)

            put(part1, lower(low, lambda a, b: lax.dot_general(a, b, (((0,), (0,)), ((), ())), preferred_element_type=jnp.float32)))
            one = GroupSum(part1, (b11, b12, b13), (s1, r1), z, c)
            one.begin()
            put(part2, lower(yv, lambda a, b: dot(a, b, ((0,), (0,)))))
            two = GroupSum(part2, (b21, b22, b23), (s2, r2), z, c)
            two.begin()
            one.middle()
            relay(sent)
            for zz in range(4):
                d_copy(1 - y, zz).wait_send()
            one.last()
            two.middle()
            one.end()

            def load(dst, ref):
                a, b, bt, d = symmetric(ref)
                dst[:LANES, :LANES] = a
                dst[LANES:, :LANES] = b
                dst[:LANES, LANES:] = bt
                dst[LANES:, LANES:] = d

            load(w, b13)

            def factor(turn, carry):
                def hook(col):
                    if col in (6 * STEP, 12 * STEP):
                        @pl.when(turn == 0)
                        def _():
                            if col == 6 * STEP:
                                two.last()
                            else:
                                two.end()
                                load(full, b23)

                inverse_factor(w, inv2, qpad, hook)

                @pl.when(turn == 0)
                def _():
                    first = inv2[...]
                    inv1[...] = first
                    w[...] = dot(dot(first, full[...]), first, ((1,), (1,)))
                return carry

            lax.fori_loop(0, 2, factor, 0)
            xs[...] = dot(ys[...], dot(inv2[...], inv1[...]), ((1,), (1,)))

        @pl.when(t == sweeps)
        def _():
            xv, zv = xs[...], acc[...]
            blocks = [dot(xv[:, i:i + LANES], zv[:, j:j + LANES], ((0,), (0,)))
                      for i in (0, LANES) for j in (0, LANES)]
            for i in range(4):
                part3[i] = blocks[i]
            three = GroupSum(part3, (b31, b32, b33), (s3, r3), z, c)
            three.begin()
            three.middle()
            relay(sent)
            for zz in range(4):
                d_copy(1 - y, zz).wait_send()
            three.last()
            three.end()
            for i in range(2):
                for j in range(2):
                    h_out[i * LANES:(i + 1) * LANES, j * LANES:(j + 1) * LANES] = b33[2 * i + j]
        return carry

    lax.fori_loop(0, sweeps + 1, sweep, 0)
    x_out[...] = xs[...]


def solution(mesh):
    if mesh.shape["row"] != 4 or mesh.shape["col"] != 4:
        raise ValueError("grid")

    def local_program(op_block, x_local, shift_vals):
        rb, bc = x_local.shape
        rows, width = op_block.shape
        f32, low = jnp.float32, jnp.bfloat16
        vmem, dma = pltpu.VMEM, pltpu.SemaphoreType.DMA
        piece, square = vmem((4, 96, LANES), f32), vmem((bc, bc), f32)
        wide = vmem((4, LANES, LANES), f32)
        return pl.pallas_call(
            functools.partial(kernel, shift_vals.shape[0]),
            out_shape=(jax.ShapeDtypeStruct((rb, bc), f32), jax.ShapeDtypeStruct((bc, bc), f32)),
            in_specs=[pl.BlockSpec(memory_space=pl.ANY), pl.BlockSpec(memory_space=pltpu.VMEM),
                      pl.BlockSpec(memory_space=pltpu.SMEM)],
            out_specs=(pl.BlockSpec(memory_space=pltpu.VMEM), pl.BlockSpec(memory_space=pltpu.VMEM)),
            scratch_shapes=[
                vmem((rb, 4 * width), low), vmem((2, 16, rb, bc), low), vmem((rb, bc), f32), vmem((rb, bc), f32),
                vmem((rb, bc), f32), square, square, square, vmem((LANES, bc), f32), square,
                piece, piece, wide, piece, piece, piece, piece, piece, piece, wide, wide, wide,
                dma((4,)), dma((4,)), dma, dma((4, 2)), dma((4, 2)), dma((4, 2)), dma((4, 2)), dma((4, 2)),
                dma((2, 4)), dma((2, 4)), dma((3, 4)), dma((3, 4)), dma((3, 4)), dma((3, 4)), dma((3, 4)), dma((3, 4)),
            ],
            compiler_params=pltpu.CompilerParams(collective_id=0, has_side_effects=True),
            name="subspace",
        )(op_block, x_local, shift_vals)

    return jax.shard_map(
        local_program, mesh=mesh,
        in_specs=(P(("batch", "row"), "col"), P(("batch", "row", "col"), None), P("batch")),
        out_specs=(P(("batch", "row", "col"), None), P("batch", None)),
        check_vma=False,
    )
```

```python
import functools

import jax
import jax.numpy as jnp
from jax import lax
from jax.experimental import pallas as pl
from jax.experimental.pallas import tpu as pltpu
from jax.sharding import PartitionSpec as P

HIGHEST = lax.Precision.HIGHEST
MESH = pl.DeviceIdType.MESH
LANES = 128
STEP = 16
LIMIT = 1e-6
GRID = ("row", "col")


def dot(a, b, dims=((1,), (0,))):
    return lax.dot_general(a, b, (dims, ((), ())), precision=HIGHEST, preferred_element_type=jnp.float32)


def inverse_factor(w, out, qpad, hook=None):
    n = w.shape[0]
    groups = n // LANES
    shape = (groups, STEP, LANES)
    rows = lax.broadcasted_iota(jnp.int32, (STEP, LANES), 0)
    spot = lax.broadcasted_iota(jnp.int32, shape, 0) * LANES + lax.broadcasted_iota(jnp.int32, shape, 2)
    qpad[...] = jnp.zeros_like(qpad)
    for k in range(0, n, STEP):
        if hook is not None:
            hook(k)
        grp, off = k // LANES, k % LANES
        panel = jnp.stack([w[k:k + STEP, g * LANES:(g + 1) * LANES] for g in range(groups)])
        cols = jnp.stack([jnp.broadcast_to(panel[grp][:, off + m:off + m + 1], (STEP, LANES)) for m in range(STEP)])
        done = []
        for j in range(STEP):
            here = (rows == j)[None]
            coef = cols[0]
            pivot = coef[j:j + 1, :]
            inv = 1.0 / pivot
            panel = jnp.where(spot == k + j, here.astype(jnp.float32), panel)
            row = panel[:, j:j + 1, :]
            done.append(row * lax.rsqrt(pivot))
            q = row * inv
            panel = jnp.where(here, q, panel - coef * q)
            if j + 1 < STEP:
                q = cols[1:, j:j + 1, :] * inv
                cols = jnp.where(here, q, cols[1:] - coef * q)
        done = jnp.concatenate(done, axis=1)
        low = k + lax.broadcasted_iota(jnp.int32, shape, 1)
        done = jnp.where(spot <= low, done, 0.0)
        for g in range(groups):
            out[k:k + STEP, g * LANES:(g + 1) * LANES] = done[g]
        if k + STEP == n:
            break
        if k:
            last = (k - STEP) % LANES
            qpad[last:last + STEP, :] = jnp.zeros((STEP, n), jnp.float32)
        for g in range(groups):
            qpad[off:off + STEP, g * LANES:(g + 1) * LANES] = panel[g]
        q = qpad[...]
        pieces = [(k + STEP, k + 2 * STEP)] + ([(k + 2 * STEP, n)] if k + 2 * STEP < n else [])
        for lo, hi in pieces:
            t = dot(w[lo:hi, grp * LANES:(grp + 1) * LANES], q)
            lane = lax.broadcasted_iota(jnp.int32, (hi - lo, n), 1)
            w[lo:hi, :] = jnp.where((lane >= k) & (lane < k + STEP), 0.0, w[lo:hi, :]) - t


def refine(a, s):
    n = a.shape[0]
    i, j = lax.broadcasted_iota(jnp.int32, (n, n), 0), lax.broadcasted_iota(jnp.int32, (n, n), 1)
    weight = jnp.where(i > j, 1.0, jnp.where(i == j, 0.5, 0.0))
    eye = jnp.where(i == j, 1.0, 0.0)
    one = weight * (dot(dot(a, s), a, ((1,), (1,))) - eye)
    b = a - dot(one - dot(one, one), a)
    two = weight * (dot(dot(b, s), b, ((1,), (1,))) - eye)
    return b - dot(two, b), jnp.sum(jnp.sum(two * two, axis=0, keepdims=True), axis=1, keepdims=True)


class GroupSum:
    def __init__(self, part, bufs, sems, z, c):
        self.part, self.z, self.c = part, z, c
        self.one, self.two, self.out = bufs
        self.send, self.recv = sems

    def _copies(self, phase):
        me = self.z if phase == 1 else self.c
        for i in range(1, 4):
            peer = lax.rem(me + i, 4)
            src = (self.part.at[peer], self.two.at[me], self.out.at[me])[phase]
            dst = (self.one, self.two, self.out)[phase].at[me]
            yield pltpu.make_async_remote_copy(
                src_ref=src, dst_ref=dst, send_sem=self.send.at[phase, i], recv_sem=self.recv.at[phase, me],
                device_id={"row": peer} if phase == 1 else {"col": peer}, device_id_type=MESH)

    def _start(self, phase):
        for copy in self._copies(phase):
            copy.start()

    def _finish(self, phase):
        me = self.z if phase == 1 else self.c
        land = (self.one, self.two, self.out)[phase]
        for i in range(1, 4):
            src = lax.rem(me + i, 4)
            pltpu.make_async_copy(land.at[src], land.at[src], self.recv.at[phase, src]).wait()
        for copy in self._copies(phase):
            copy.wait_send()

    def begin(self):
        self._start(0)

    def middle(self):
        self._finish(0)
        self.one[self.c] = self.part[self.c]
        self.two[self.z] = (self.one[0] + self.one[1]) + (self.one[2] + self.one[3])
        self._start(1)

    def last(self):
        self._finish(1)
        self.out[self.c] = (self.two[0] + self.two[1]) + (self.two[2] + self.two[3])
        self._start(2)

    def end(self):
        self._finish(2)


def symmetric(ref):
    flat = ref[...].reshape(3 * LANES, LANES)
    a, b, c = flat[:LANES], flat[LANES:2 * LANES], flat[2 * LANES:]
    return a, b, b.T, c


def kernel(sweeps, a_hbm, x0, sigma, x_out, h_out, bad_out, arows, xg, acc, xs, ys, w, inv1, qpad, full, worst, flags,
           part1, part2, part3, b11, b12, b13, b21, b22, b23, b31, b32, b33,
           asend, arecv, aown, up, down, zrecv, ysend, yrecv, dsend, drecv,
           s1, r1, s2, r2, s3, r3, fsend, frecv):
    z, c = lax.axis_index("row"), lax.axis_index("col")
    y, k = c // 2, lax.rem(c, 2)
    rb, bc = x0.shape
    half = rb // 2
    width = a_hbm.shape[1]
    twin = c + 1 - 2 * k
    across = lax.rem(c + 2, 4)

    barrier = pltpu.get_barrier_semaphore()
    for i in range(1, 4):
        pl.semaphore_signal(barrier, inc=1, device_id={"col": lax.rem(c + i, 4)}, device_id_type=MESH)
        pl.semaphore_signal(barrier, inc=1, device_id={"row": lax.rem(z + i, 4)}, device_id_type=MESH)
    other = 1 - lax.axis_index("batch")
    pl.semaphore_signal(barrier, inc=1, device_id={"batch": other}, device_id_type=MESH)
    pl.semaphore_wait(barrier, 7)

    def columns(block):
        return pl.ds(pl.multiple_of(block * width, LANES), width)

    def spread(i):
        peer = lax.rem(c + i, 4)
        return pltpu.make_async_remote_copy(
            src_ref=a_hbm.at[pl.ds(pl.multiple_of(peer * rb, STEP), rb)], dst_ref=arows.at[:, columns(c)],
            send_sem=asend.at[i], recv_sem=arecv.at[c], device_id={"col": peer}, device_id_type=MESH)

    own_rows = pltpu.make_async_copy(a_hbm.at[pl.ds(pl.multiple_of(c * rb, STEP), rb)], arows.at[:, columns(c)], aown)
    for i in range(1, 4):
        spread(i).start()
    own_rows.start()
    xs[...] = x0[...]
    worst[...] = jnp.zeros_like(worst)
    def sweep(t, carry):
        p = lax.rem(t, 2)

        def shard(yy, zz, kk):
            return xg.at[p, zz * 4 + yy * 2 + kk]

        def piece(yy, zz, kk, h):
            return xg.at[p, zz * 4 + yy * 2 + kk, pl.ds(h * half, half)]

        def z_copy(zz, h, step):
            sems = up if step > 0 else down
            return pltpu.make_async_remote_copy(
                src_ref=piece(y, zz, k, h), dst_ref=piece(y, zz, k, h), send_sem=sems.at[zz, h],
                recv_sem=zrecv.at[zz, h], device_id={"row": z + step}, device_id_type=MESH)

        def y_copy(zz, h):
            return pltpu.make_async_remote_copy(
                src_ref=piece(y, zz, k, h), dst_ref=piece(y, zz, k, h), send_sem=ysend.at[zz, h],
                recv_sem=yrecv.at[zz, h], device_id={"col": across}, device_id_type=MESH)

        def d_copy(yy, zz):
            return pltpu.make_async_remote_copy(
                src_ref=shard(yy, zz, k), dst_ref=shard(yy, zz, k), send_sem=dsend.at[yy, zz],
                recv_sem=drecv.at[yy, zz], device_id={"col": twin}, device_id_type=MESH)

        def landed(ref, sem):
            pltpu.make_async_copy(ref, ref, sem).wait()

        def relay(act):
            for h in range(2):
                for step, ok in ((1, z < 3), (-1, z > 0)):
                    @pl.when(ok)
                    def _():
                        act(z_copy(z, h, step))
                act(y_copy(z, h))
            act(d_copy(y, z))
            for d in range(1, 4):
                for step, there, on in ((1, z >= d, z < 3), (-1, z + d <= 3, z > 0)):
                    @pl.when(there)
                    def _():
                        zz = z - step * d
                        for h in range(2):
                            if act is start:
                                landed(piece(y, zz, k, h), zrecv.at[zz, h])

                            @pl.when(on)
                            def _():
                                act(z_copy(zz, h, step))
                            act(y_copy(zz, h))
                        act(d_copy(y, zz))

        def start(copy):
            copy.start()

        def sent(copy):
            copy.wait_send()

        def near(i):
            return lax.rem(z // 2 + i // 2, 2) * 2 + lax.rem(lax.rem(z, 2) + lax.rem(i, 2), 2)

        def consume(yy, zz):
            block = zz * 4 + yy * 2
            cols = pl.ds(pl.multiple_of(block * rb, LANES), 2 * rb)
            acc[...] += jnp.dot(arows[:, cols], xg[p, pl.ds(block, 2)].reshape(2 * rb, bc), preferred_element_type=jnp.float32)

        xg[p, z * 4 + c] = xs[...].astype(jnp.bfloat16)
        relay(start)
        acc[...] = jnp.zeros_like(acc)

        @pl.when(t == 0)
        def _():
            own_rows.wait()
            for i in range(1, 4):
                src = lax.rem(c + i, 4)
                landed(arows.at[:, columns(src)], arecv.at[src])
            for i in range(1, 4):
                spread(i).wait_send()

        def same_plane(i, carry):
            zz = near(i)
            landed(shard(y, zz, 1 - k), drecv.at[y, zz])
            consume(y, zz)
            return carry

        def other_plane(i, carry):
            zz = near(i)
            for h in range(2):
                landed(piece(1 - y, zz, k, h), yrecv.at[zz, h])
            d_copy(1 - y, zz).start()
            landed(shard(1 - y, zz, 1 - k), drecv.at[1 - y, zz])
            consume(1 - y, zz)
            return carry

        lax.fori_loop(0, 4, same_plane, 0)
        lax.fori_loop(0, 4, other_plane, 0)

        @pl.when(t < sweeps)
        def _():
            shift = sigma[lax.rem(t, sweeps)]
            yv = acc[...] - shift * xs[...]
            ys[...] = yv
            low = yv.astype(jnp.bfloat16)

            def lower(v, mul):
                v0, v1 = v[:, :LANES], v[:, LANES:]
                return [mul(a, b).reshape(LANES, LANES) for a, b in ((v0, v0), (v1, v0), (v1, v1))]

            def put(part, blocks):
                part[...] = jnp.concatenate(blocks, axis=0).reshape(part.shape)

            put(part1, lower(low, lambda a, b: lax.dot_general(a, b, (((0,), (0,)), ((), ())), preferred_element_type=jnp.float32)))
            one = GroupSum(part1, (b11, b12, b13), (s1, r1), z, c)
            one.begin()
            put(part2, lower(yv, lambda a, b: dot(a, b, ((0,), (0,)))))
            two = GroupSum(part2, (b21, b22, b23), (s2, r2), z, c)
            two.begin()
            one.middle()
            relay(sent)
            for zz in range(4):
                d_copy(1 - y, zz).wait_send()
            one.last()
            two.middle()
            one.end()

            def load(dst, ref):
                a, b, bt, d = symmetric(ref)
                dst[:LANES, :LANES] = a
                dst[LANES:, :LANES] = b
                dst[:LANES, LANES:] = bt
                dst[LANES:, LANES:] = d

            def hook(col):
                if col == 6 * STEP:
                    two.last()
                if col == 12 * STEP:
                    two.end()
                    load(full, b23)

            load(w, b13)
            inverse_factor(w, inv1, qpad, hook)
            inverse, left = refine(inv1[...], full[...])
            xs[...] = dot(ys[...], inverse, ((1,), (1,)))
            worst[...] = worst[...] + jnp.where(left <= LIMIT, 0.0, 1.0)

        @pl.when(t == sweeps)
        def _():
            flags[1 - other] = worst[...]
            tell = pltpu.make_async_remote_copy(
                src_ref=flags.at[1 - other], dst_ref=flags.at[1 - other], send_sem=fsend, recv_sem=frecv,
                device_id={"batch": other}, device_id_type=MESH)
            tell.start()
            xv, zv = xs[...], acc[...]
            blocks = [dot(xv[:, i:i + LANES], zv[:, j:j + LANES], ((0,), (0,)))
                      for i in (0, LANES) for j in (0, LANES)]
            for i in range(4):
                part3[i] = blocks[i]
            three = GroupSum(part3, (b31, b32, b33), (s3, r3), z, c)
            three.begin()
            three.middle()
            relay(sent)
            for zz in range(4):
                d_copy(1 - y, zz).wait_send()
            three.last()
            three.end()
            landed(flags.at[other], frecv)
            tell.wait_send()
            bad_out[...] = flags[0] + flags[1]
            for i in range(2):
                for j in range(2):
                    h_out[i * LANES:(i + 1) * LANES, j * LANES:(j + 1) * LANES] = b33[2 * i + j]
        return carry

    lax.fori_loop(0, sweeps + 1, sweep, 0)
    x_out[...] = xs[...]


def plain_program(op_block, x_local, shift_vals):
    moves = [(i, (i % 4) * 4 + i // 4) for i in range(16)]

    def apply_block(x_local):
        x_moved = lax.ppermute(x_local.astype(jnp.bfloat16), GRID, moves)
        x_column = lax.all_gather(x_moved, "row", axis=0, tiled=True)
        part_sum = jnp.dot(op_block, x_column, preferred_element_type=jnp.float32)
        return lax.psum_scatter(part_sum, "col", scatter_dimension=0, tiled=True)

    def orthonormalize(turn, y_local):
        low = y_local.astype(jnp.bfloat16)
        gram_one = jnp.einsum("ka,kb->ab", low, low, preferred_element_type=jnp.float32)
        gram_two = jnp.einsum("ka,kb->ab", y_local, y_local, precision=HIGHEST, preferred_element_type=jnp.float32)
        lower = jnp.linalg.cholesky(lax.psum(jnp.where(turn == 0, gram_one, gram_two), GRID))
        return lax.linalg.triangular_solve(lower, y_local, left_side=False, lower=True, transpose_a=True)

    def sweep(step, x_local):
        y_local = apply_block(x_local) - shift_vals[step] * x_local
        return lax.fori_loop(0, 2, orthonormalize, y_local)

    x_local = lax.fori_loop(0, shift_vals.shape[0], sweep, x_local)
    image = apply_block(x_local)
    local_gram = jnp.einsum("ka,kb->ab", x_local, image, precision=HIGHEST, preferred_element_type=jnp.float32)
    return x_local, lax.psum(local_gram, GRID)


def solution(mesh):
    if mesh.shape["row"] != 4 or mesh.shape["col"] != 4:
        raise ValueError("grid")

    def local_program(op_block, x_local, shift_vals):
        rb, bc = x_local.shape
        rows, width = op_block.shape
        f32, low = jnp.float32, jnp.bfloat16
        vmem, dma = pltpu.VMEM, pltpu.SemaphoreType.DMA
        piece, square = vmem((4, 96, LANES), f32), vmem((bc, bc), f32)
        wide = vmem((4, LANES, LANES), f32)
        x_fast, h_fast, bad = pl.pallas_call(
            functools.partial(kernel, shift_vals.shape[0]),
            out_shape=(jax.ShapeDtypeStruct((rb, bc), f32), jax.ShapeDtypeStruct((bc, bc), f32),
                       jax.ShapeDtypeStruct((8, LANES), f32)),
            in_specs=[pl.BlockSpec(memory_space=pl.ANY), pl.BlockSpec(memory_space=pltpu.VMEM),
                      pl.BlockSpec(memory_space=pltpu.SMEM)],
            out_specs=(pl.BlockSpec(memory_space=pltpu.VMEM),) * 3,
            scratch_shapes=[
                vmem((rb, 4 * width), low), vmem((2, 16, rb, bc), low), vmem((rb, bc), f32), vmem((rb, bc), f32),
                vmem((rb, bc), f32), square, square, vmem((LANES, bc), f32), square, vmem((8, LANES), f32), vmem((2, 8, LANES), f32),
                piece, piece, wide, piece, piece, piece, piece, piece, piece, wide, wide, wide,
                dma((4,)), dma((4,)), dma, dma((4, 2)), dma((4, 2)), dma((4, 2)), dma((4, 2)), dma((4, 2)),
                dma((2, 4)), dma((2, 4)), dma((3, 4)), dma((3, 4)), dma((3, 4)), dma((3, 4)), dma((3, 4)), dma((3, 4)), dma, dma,
            ],
            compiler_params=pltpu.CompilerParams(collective_id=0, has_side_effects=True),
            name="subspace",
        )(op_block, x_local, shift_vals)
        return lax.cond(bad[0, 0] == 0.0, lambda *args: (x_fast, h_fast), plain_program, op_block, x_local, shift_vals)

    return jax.shard_map(
        local_program, mesh=mesh,
        in_specs=(P(("batch", "row"), "col"), P(("batch", "row", "col"), None), P("batch")),
        out_specs=(P(("batch", "row", "col"), None), P("batch", None)),
        check_vma=False,
    )
```
